32 devices in a mesh: section: 4 (over y, x), fsdp: 8 (over z, core).
Axes of the slice: x: 2, y: 2, z: 4, core: 2. Of those that a mesh axis runs over, the one named last changes fastest.
Arguments:
- master: float32 [4, 64, 4096], P('section', 'fsdp'), may hold values from -0.12 to 0.12
- first_moment: float32 [4, 64, 4096], P('section', 'fsdp'), may hold values from -0.2 to 0.2
- second_moment: float32 [4, 64, 4096], P('section', 'fsdp'), may hold values from 0.25 to 1
- gradient: float32 [4, 64, 4096], P('section', 'fsdp'), may hold values from -64 to 64
Outputs:
- new_master: float32 [4, 64, 4096], P('section', 'fsdp')
- new_first: float32 [4, 64, 4096], P('section', 'fsdp')
- new_second: float32 [4, 64, 4096], P('section', 'fsdp')
- weights: bfloat16 [4, 64, 4096], P('section')
- grad_rms: float32 [], replicated
The draws below stay inside these ranges and needn't reach their ends.
All inputs are finite; a program needn't handle non-finite values.
Results may differ from the reference program's by a relative error of at most 0.001.
Values may be sent and summed in bfloat16 or wider, within the bound.
A program may use at most 64 MiB of HBM per device.

```python
import math
import jax
import jax.numpy as jnp

D = 4096
ROWS_DEV = 8
ROWS = 64
SECTIONS = 4


def draw_gradient(key, part):
    key_base = jax.random.fold_in(key, 11)
    key_rows = jax.random.fold_in(key, 12)
    key_blocks = jax.random.fold_in(key, 13)
    base = jnp.clip(jax.random.normal(key_base, (SECTIONS, ROWS, D), jnp.float32), -6.0, 6.0)
    row_scale = jnp.exp(jax.random.uniform(key_rows, (SECTIONS, ROWS, 1), jnp.float32, jnp.log(0.5), jnp.log(2.0)))
    common = jnp.zeros((1, 1, D), jnp.float32)
    block_scale = jnp.exp(jax.random.uniform(key_blocks, (SECTIONS, ROWS // ROWS_DEV, 1, 1), jnp.float32, jnp.log(0.5), jnp.log(2.0)))
    block_scale = jnp.broadcast_to(block_scale, (SECTIONS, ROWS // ROWS_DEV, ROWS_DEV, 1)).reshape(SECTIONS, ROWS, 1)
    return base * row_scale * block_scale + common


def shard_levels(own_key, shape, split, smallest, largest):
    def one(position, parts):
        heights = jax.random.uniform(jax.random.fold_in(jax.random.fold_in(own_key, 6), position), (parts,), jnp.float32, smallest / len(split), largest / len(split))
        return jnp.repeat(jnp.exp(heights), shape[position] // parts).reshape((-1,) + (1,) * (len(shape) - position - 1))

    gain = one(*split[0])
    for cut in split[1:]:
        gain = gain * one(*cut)
    return gain


def centred(key, shape, deviation, bound, split=(), dtype=jnp.bfloat16):
    array = jax.random.normal(key, shape, jnp.float32) * deviation
    if len(split) > 0:
        array = shard_levels(key, shape, split, -0.22, 0.18) * array
    return jnp.clip(array, min=-bound, max=bound).astype(dtype)


def setup_inputs(seed: int = 0) -> dict:
    seeds = jax.random.split(jax.random.key(seed), 5)
    return {
        "master": centred(seeds[0], (SECTIONS, ROWS, D), 0.02, 0.12, ((0, 4), (1, 8)), jnp.float32),
        "first_moment": centred(seeds[1], (SECTIONS, ROWS, D), 0.05, 0.2, ((0, 4), (1, 8)), jnp.float32),
        "second_moment": jnp.clip(jnp.exp(math.log(1.0) - 1.3862944 * jax.random.uniform(seeds[2], (SECTIONS, ROWS, D), jnp.float32) ** shard_levels(seeds[2], (SECTIONS, ROWS, D), ((0, 4), (1, 8)), -0.2, 0.2)), 0.25, 1.0),
        "gradient": draw_gradient(jax.random.fold_in(seeds[4], 71), 0),
    }


BETA_ONE = 0.9
BETA_TWO = 0.95
LEARN_RATE = 0.05
DECAY = 0.1
EPSILON = 1e-08
BIAS_STEPS = 10.0

def reference(master, first_moment, second_moment, gradient):
    squares = jnp.sum(gradient * gradient)
    grad_norm = jnp.sqrt(squares)
    param_count = float(SECTIONS * ROWS * D)
    limit = jnp.float32(0.5 * param_count ** 0.5)
    clip_scale = limit / jnp.maximum(grad_norm, limit)
    scaled = clip_scale * gradient
    new_first = BETA_ONE * first_moment + (1.0 - BETA_ONE) * scaled
    new_second = BETA_TWO * second_moment + (1.0 - BETA_TWO) * scaled * scaled
    first_hat = new_first / (1.0 - BETA_ONE ** BIAS_STEPS)
    second_hat = new_second / (1.0 - BETA_TWO ** BIAS_STEPS)
    update = first_hat / (jnp.sqrt(second_hat) + EPSILON)
    new_master = master * (1.0 - LEARN_RATE * DECAY) - LEARN_RATE * update
    grad_rms = grad_norm / jnp.float32(param_count ** 0.5)
    return (new_master, new_first, new_second, new_master.astype(jnp.bfloat16), grad_rms)
```

```python
import functools

import jax
import jax.numpy as jnp
from jax import lax
from jax.experimental import pallas as pl
from jax.experimental.pallas import tpu as pltpu
from jax.sharding import PartitionSpec as P

BETA_ONE = 0.9
BETA_TWO = 0.95
LEARN_RATE = 0.05
DECAY = 0.1
EPSILON = 1e-08
BIAS_STEPS = 10.0
MESH = pl.DeviceIdType.MESH
UNROLL_MOST = 128


def for_each(count, body):
    if count <= UNROLL_MOST:
        for i in range(count):
            body(i)
    else:
        lax.fori_loop(0, count, lambda i, carry: (body(i), carry)[1], 0)


def step_kernel(
    sections, shards, params,
    master_hbm, first_hbm, second_hbm, grad_hbm,
    new_master, new_first, new_second, weights, rms,
    master, first, second, grad, part, parts,
    load_sem, part_send, part_recv, block_send, block_recv, pair_send,
):
    my_section = lax.axis_index("section")
    my_shard = lax.axis_index("fsdp")
    total = sections * shards
    me = my_section * shards + my_shard

    loads = [
        pltpu.make_async_copy(src.at[0], dst, load_sem.at[i])
        for i, (src, dst) in enumerate(
            ((grad_hbm, grad), (master_hbm, master), (first_hbm, first), (second_hbm, second))
        )
    ]
    for load in loads:
        load.start()

    def peer(i):
        s = lax.rem(my_section + i // shards, sections)
        f = lax.rem(my_shard + i % shards, shards)
        return s, f

    barrier = pltpu.get_barrier_semaphore()

    def greet(i):
        pl.semaphore_signal(barrier, inc=1, device_id=peer(i + 1), device_id_type=MESH)

    for_each(total - 1, greet)

    loads[0].wait()
    g = grad[...]
    squares = g * g
    width = squares.shape[1]
    folded = squares[:, :128]
    for j in range(1, width // 128):
        folded += squares[:, j * 128 : (j + 1) * 128]
    row = jnp.sum(folded, axis=0, keepdims=True)
    part[...] = row
    parts[pl.ds(me, 1), :] = row

    pl.semaphore_wait(barrier, total - 1)

    def send_part(i):
        s, f = peer(i + 1)
        pltpu.make_async_remote_copy(
            src_ref=part,
            dst_ref=parts.at[pl.ds(me, 1)],
            send_sem=part_send,
            recv_sem=part_recv,
            device_id=(s, f),
            device_id_type=MESH,
        ).start()

    for_each(total - 1, send_part)
    for load in loads[1:]:
        load.wait()
    others = parts.at[pl.ds(0, total - 1)]
    pltpu.make_async_copy(others, others, part_recv).wait()

    squares_all = jnp.sum(jnp.sum(parts[...], axis=0, keepdims=True), axis=1, keepdims=True)
    norm = jnp.sqrt(squares_all)
    limit = jnp.float32(0.5 * params**0.5)
    clip = limit / jnp.maximum(norm, limit)
    rms[...] = norm / jnp.float32(params**0.5)

    scaled = clip * g
    nf = BETA_ONE * first[...] + (1.0 - BETA_ONE) * scaled
    ns = BETA_TWO * second[...] + (1.0 - BETA_TWO) * scaled * scaled
    first_hat = nf / (1.0 - BETA_ONE**BIAS_STEPS)
    second_hat = ns / (1.0 - BETA_TWO**BIAS_STEPS)
    update = first_hat / (jnp.sqrt(second_hat) + EPSILON)
    nm = master[...] * (1.0 - LEARN_RATE * DECAY) - LEARN_RATE * update
    weights[my_shard] = nm.astype(jnp.bfloat16)
    new_master[0] = nm
    new_first[0] = nf
    new_second[0] = ns

    cores = 2 if shards % 2 == 0 else 1
    chips = shards // cores
    core = my_shard % cores
    chip = my_shard // cores
    partner = chip * cores + (cores - 1 - core)

    def to(block, shard, send_sem):
        return pltpu.make_async_remote_copy(
            src_ref=weights.at[block],
            dst_ref=weights.at[block],
            send_sem=send_sem,
            recv_sem=block_recv.at[block],
            device_id=(my_section, shard),
            device_id_type=MESH,
        )

    def across(i):
        other = lax.rem(chip + i + 1, chips) * cores + core
        to(my_shard, other, block_send.at[i]).start()

    for_each(chips - 1, across)
    if cores == 2:
        to(my_shard, partner, pair_send.at[chips - 1]).start()

    def arrived(i):
        block = lax.rem(chip + chips - i - 1, chips) * cores + core
        to(block, partner, block_send.at[i]).wait_recv()
        if cores == 2:
            to(block, partner, pair_send.at[i]).start()

    for_each(chips - 1, arrived)
    if cores == 2:

        def arrived_pair(i):
            block = lax.rem(chip + chips - i - 1, chips) * cores + (1 - core)
            to(block, partner, pair_send.at[i]).wait_recv()

        for_each(chips, arrived_pair)

        def sent_pair(i):
            to(my_shard, partner, pair_send.at[i]).wait_send()

        for_each(chips, sent_pair)

    def sent(i):
        to(my_shard, partner, block_send.at[i]).wait_send()

    for_each(chips - 1, sent)
    pltpu.make_async_copy(others, others, part_send).wait()


def local(sections, shards, master, first_moment, second_moment, gradient):
    _, rows, width = gradient.shape
    params = float(sections * shards * rows * width)
    total = sections * shards
    chips = max(shards // 2, 1) if shards % 2 == 0 else shards
    vmem = pl.BlockSpec(memory_space=pltpu.VMEM)
    hbm = pl.BlockSpec(memory_space=pl.ANY)
    block = jax.ShapeDtypeStruct((1, rows, width), jnp.float32)
    new_master, new_first, new_second, weights, rms = pl.pallas_call(
        functools.partial(step_kernel, sections, shards, params),
        out_shape=(
            block,
            block,
            block,
            jax.ShapeDtypeStruct((shards, rows, width), jnp.bfloat16),
            jax.ShapeDtypeStruct((1, 1), jnp.float32),
        ),
        in_specs=[hbm] * 4,
        out_specs=(vmem,) * 5,
        scratch_shapes=[pltpu.VMEM((rows, width), jnp.float32)] * 4
        + [
            pltpu.VMEM((1, 128), jnp.float32),
            pltpu.VMEM((total, 128), jnp.float32),
            pltpu.SemaphoreType.DMA((4,)),
            pltpu.SemaphoreType.DMA,
            pltpu.SemaphoreType.DMA,
            pltpu.SemaphoreType.DMA((chips,)),
            pltpu.SemaphoreType.DMA((shards,)),
            pltpu.SemaphoreType.DMA((chips,)),
        ],
        compiler_params=pltpu.CompilerParams(collective_id=0, has_side_effects=True),
    )(master, first_moment, second_moment, gradient)
    return (
        new_master,
        new_first,
        new_second,
        weights.reshape(1, shards * rows, width),
        rms.reshape(()),
    )


def solution(mesh):
    placed = (P("section", "fsdp", None),) * 4
    return jax.shard_map(
        functools.partial(local, mesh.shape["section"], mesh.shape["fsdp"]),
        mesh=mesh,
        in_specs=placed,
        out_specs=(
            P("section", "fsdp", None),
            P("section", "fsdp", None),
            P("section", "fsdp", None),
            P("section", None, None),
            P(),
        ),
        check_vma=False,
    )
```

```python
import functools

import jax
import jax.numpy as jnp
from jax import lax
from jax.experimental import pallas as pl
from jax.experimental.pallas import tpu as pltpu
from jax.sharding import PartitionSpec as P

BETA_ONE = 0.9
BETA_TWO = 0.95
LEARN_RATE = 0.05
DECAY = 0.1
EPSILON = 1e-08
BIAS_STEPS = 10.0
MESH = pl.DeviceIdType.MESH
UNROLL_MOST = 128
VMEM_GRANT = 16 * 1024 * 1024


def for_each(count, body):
    if count <= UNROLL_MOST:
        for i in range(count):
            body(i)
    else:
        lax.fori_loop(0, count, lambda i, carry: (body(i), carry)[1], 0)


def step_kernel(
    sections, shards, params,
    master_hbm, first_hbm, second_hbm, grad_hbm,
    new_master, new_first, new_second, weights, rms,
    master, first, second, grad, part, parts,
    load_sem, part_send, part_recv, block_send, block_recv, pair_send,
):
    my_section = lax.axis_index("section")
    my_shard = lax.axis_index("fsdp")
    total = sections * shards
    me = my_section * shards + my_shard

    loads = [
        pltpu.make_async_copy(src.at[0], dst, load_sem.at[i])
        for i, (src, dst) in enumerate(
            ((grad_hbm, grad), (master_hbm, master), (first_hbm, first), (second_hbm, second))
        )
    ]
    for load in loads:
        load.start()

    def peer(i):
        s = lax.rem(my_section + i // shards, sections)
        f = lax.rem(my_shard + i % shards, shards)
        return s, f

    barrier = pltpu.get_barrier_semaphore()

    def greet(i):
        pl.semaphore_signal(barrier, inc=1, device_id=peer(i + 1), device_id_type=MESH)

    for_each(total - 1, greet)

    loads[0].wait()
    g = grad[...]
    squares = g * g
    width = squares.shape[1]
    folded = squares[:, :128]
    for j in range(1, width // 128):
        folded += squares[:, j * 128 : (j + 1) * 128]
    row = jnp.sum(folded, axis=0, keepdims=True)
    part[...] = row
    parts[pl.ds(me, 1), :] = row

    pl.semaphore_wait(barrier, total - 1)

    def send_part(i):
        s, f = peer(i + 1)
        pltpu.make_async_remote_copy(
            src_ref=part,
            dst_ref=parts.at[pl.ds(me, 1)],
            send_sem=part_send,
            recv_sem=part_recv,
            device_id=(s, f),
            device_id_type=MESH,
        ).start()

    for_each(total - 1, send_part)
    for load in loads[1:]:
        load.wait()
    others = parts.at[pl.ds(0, total - 1)]
    pltpu.make_async_copy(others, others, part_recv).wait()

    squares_all = jnp.sum(jnp.sum(parts[...], axis=0, keepdims=True), axis=1, keepdims=True)
    norm = jnp.sqrt(squares_all)
    limit = jnp.float32(0.5 * params**0.5)
    clip = limit / jnp.maximum(norm, limit)
    rms[...] = norm / jnp.float32(params**0.5)

    scaled = clip * g
    nf = BETA_ONE * first[...] + (1.0 - BETA_ONE) * scaled
    ns = BETA_TWO * second[...] + (1.0 - BETA_TWO) * scaled * scaled
    first_hat = nf / (1.0 - BETA_ONE**BIAS_STEPS)
    second_hat = ns / (1.0 - BETA_TWO**BIAS_STEPS)
    update = first_hat / (jnp.sqrt(second_hat) + EPSILON)
    nm = master[...] * (1.0 - LEARN_RATE * DECAY) - LEARN_RATE * update
    weights[my_shard] = nm.astype(jnp.bfloat16)
    new_master[0] = nm
    new_first[0] = nf
    new_second[0] = ns

    cores = 2 if shards % 2 == 0 else 1
    chips = shards // cores
    core = my_shard % cores
    chip = my_shard // cores
    partner = chip * cores + (cores - 1 - core)

    def to(block, shard, send_sem):
        return pltpu.make_async_remote_copy(
            src_ref=weights.at[block],
            dst_ref=weights.at[block],
            send_sem=send_sem,
            recv_sem=block_recv.at[block],
            device_id=(my_section, shard),
            device_id_type=MESH,
        )

    def across(i):
        other = lax.rem(chip + i + 1, chips) * cores + core
        to(my_shard, other, block_send.at[i]).start()

    for_each(chips - 1, across)
    if cores == 2:
        to(my_shard, partner, pair_send.at[chips - 1]).start()

    def arrived(i):
        block = lax.rem(chip + chips - i - 1, chips) * cores + core
        to(block, partner, block_send.at[i]).wait_recv()
        if cores == 2:
            to(block, partner, pair_send.at[i]).start()

    for_each(chips - 1, arrived)
    if cores == 2:

        def arrived_pair(i):
            block = lax.rem(chip + chips - i - 1, chips) * cores + (1 - core)
            to(block, partner, pair_send.at[i]).wait_recv()

        for_each(chips, arrived_pair)

        def sent_pair(i):
            to(my_shard, partner, pair_send.at[i]).wait_send()

        for_each(chips, sent_pair)

    def sent(i):
        to(my_shard, partner, block_send.at[i]).wait_send()

    for_each(chips - 1, sent)
    pltpu.make_async_copy(others, others, part_send).wait()


def store_kernel(*refs):
    count = len(refs) // 2
    copies = [
        pltpu.make_async_copy(refs[i], refs[count + i], refs[-1].at[i]) for i in range(count)
    ]
    for copy in copies:
        copy.start()
    for copy in copies:
        copy.wait()


def local(sections, shards, master, first_moment, second_moment, gradient):
    _, rows, width = gradient.shape
    params = float(sections * shards * rows * width)
    total = sections * shards
    chips = max(shards // 2, 1) if shards % 2 == 0 else shards
    vmem = pl.BlockSpec(memory_space=pltpu.VMEM)
    hbm = pl.BlockSpec(memory_space=pl.ANY)
    results = [((1, rows, width), jnp.float32)] * 3
    results += [((shards, rows, width), jnp.bfloat16), ((1, 1), jnp.float32)]
    held = pl.pallas_call(
        functools.partial(step_kernel, sections, shards, params),
        out_shape=tuple(pltpu.VMEM(shape, dtype) for shape, dtype in results),
        in_specs=[hbm] * 4,
        out_specs=(vmem,) * 5,
        scratch_shapes=[pltpu.VMEM((rows, width), jnp.float32)] * 4
        + [
            pltpu.VMEM((1, 128), jnp.float32),
            pltpu.VMEM((total, 128), jnp.float32),
            pltpu.SemaphoreType.DMA((4,)),
            pltpu.SemaphoreType.DMA,
            pltpu.SemaphoreType.DMA,
            pltpu.SemaphoreType.DMA((chips,)),
            pltpu.SemaphoreType.DMA((shards,)),
            pltpu.SemaphoreType.DMA((chips,)),
        ],
        compiler_params=pltpu.CompilerParams(
            collective_id=0, has_side_effects=True, vmem_limit_bytes=VMEM_GRANT
        ),
    )(master, first_moment, second_moment, gradient)
    new_master, new_first, new_second, weights, rms = pl.pallas_call(
        store_kernel,
        out_shape=tuple(jax.ShapeDtypeStruct(shape, dtype) for shape, dtype in results),
        in_specs=[vmem] * 5,
        out_specs=(hbm,) * 5,
        scratch_shapes=[pltpu.SemaphoreType.DMA((5,))],
        compiler_params=pltpu.CompilerParams(vmem_limit_bytes=VMEM_GRANT),
    )(*[pltpu.with_memory_space_constraint(x, pltpu.VMEM) for x in held])
    return (
        new_master,
        new_first,
        new_second,
        weights.reshape(1, shards * rows, width),
        rms.reshape(()),
    )


def solution(mesh):
    placed = (P("section", "fsdp", None),) * 4
    return jax.shard_map(
        functools.partial(local, mesh.shape["section"], mesh.shape["fsdp"]),
        mesh=mesh,
        in_specs=placed,
        out_specs=(
            P("section", "fsdp", None),
            P("section", "fsdp", None),
            P("section", "fsdp", None),
            P("section", None, None),
            P(),
        ),
        check_vma=False,
    )
```

```python
import functools
import math

import jax
import jax.numpy as jnp
from jax import lax
from jax.experimental import pallas as pl
from jax.experimental.pallas import tpu as pltpu
from jax.sharding import PartitionSpec as P

BETA_ONE = 0.9
BETA_TWO = 0.95
LEARN_RATE = 0.05
DECAY = 0.1
EPSILON = 1e-08
BIAS_STEPS = 10.0
MESH = pl.DeviceIdType.MESH
UNROLL_MOST = 40
PIECES = 1
VMEM_MOST = 67043328
GRANT_MOST = 60 * 1024 * 1024


def for_each(count, body):
    if count <= UNROLL_MOST:
        for i in range(count):
            body(i)
    else:
        lax.fori_loop(0, count, lambda i, carry: (body(i), carry)[1], 0)


def step_kernel(
    sections, shards, params, pieces,
    master_hbm, first_hbm, second_hbm, grad_hbm,
    new_master, new_first, new_second, weights, rms,
    master, first, second, grad, part, parts,
    load_sem, part_send, part_recv, line_send, line_recv, pair_send, pair_recv,
):
    my_section = lax.axis_index("section")
    my_shard = lax.axis_index("fsdp")
    total = sections * shards
    me = my_section * shards + my_shard

    loads = [
        pltpu.make_async_copy(src.at[0], dst, load_sem.at[i])
        for i, (src, dst) in enumerate(
            ((grad_hbm, grad), (master_hbm, master), (first_hbm, first), (second_hbm, second))
        )
    ]
    loads[0].start()

    def peer(i):
        s = lax.rem(my_section + i // shards, sections)
        f = lax.rem(my_shard + i % shards, shards)
        return s, f

    barrier = pltpu.get_barrier_semaphore()

    def greet(i):
        pl.semaphore_signal(barrier, inc=1, device_id=peer(i + 1), device_id_type=MESH)

    for_each(total - 1, greet)

    for load in loads[1:]:
        load.start()

    loads[0].wait()
    g = grad[...]
    squares = g * g
    width = squares.shape[1]
    folded = squares[:, :128]
    for j in range(1, width // 128):
        folded += squares[:, j * 128 : (j + 1) * 128]
    row = jnp.sum(folded, axis=0, keepdims=True)
    part[...] = row
    parts[pl.ds(me, 1), :] = row

    pl.semaphore_wait(barrier, total - 1)

    def send_part(i):
        s, f = peer(i + 1)
        pltpu.make_async_remote_copy(
            src_ref=part,
            dst_ref=parts.at[pl.ds(me, 1)],
            send_sem=part_send,
            recv_sem=part_recv,
            device_id=(s, f),
            device_id_type=MESH,
        ).start()

    for_each(total - 1, send_part)
    for load in loads[1:]:
        load.wait()
    others = parts.at[pl.ds(0, total - 1)]
    pltpu.make_async_copy(others, others, part_recv).wait()

    squares_all = jnp.sum(jnp.sum(parts[...], axis=0, keepdims=True), axis=1, keepdims=True)
    norm = jnp.sqrt(squares_all)
    limit = jnp.float32(0.5 * params**0.5)
    clip = limit / jnp.maximum(norm, limit)
    rms[...] = norm / jnp.float32(params**0.5)

    scaled = clip * g
    nf = BETA_ONE * first[...] + (1.0 - BETA_ONE) * scaled
    ns = BETA_TWO * second[...] + (1.0 - BETA_TWO) * scaled * scaled
    first_hat = nf / (1.0 - BETA_ONE**BIAS_STEPS)
    second_hat = ns / (1.0 - BETA_TWO**BIAS_STEPS)
    update = first_hat / (jnp.sqrt(second_hat) + EPSILON)
    nm = master[...] * (1.0 - LEARN_RATE * DECAY) - LEARN_RATE * update
    weights[my_shard] = nm.astype(jnp.bfloat16)
    new_master[0] = nm
    new_first[0] = nf
    new_second[0] = ns

    cores = 2 if shards % 2 == 0 else 1
    chips = shards // cores
    core = my_shard % cores
    chip = my_shard // cores
    pair = 1 - core
    cut = width // pieces

    def copy(block, piece, shard, send_sem, recv_sem):
        there = weights.at[block, :, pl.ds(piece * cut, cut)]
        return pltpu.make_async_remote_copy(
            src_ref=there,
            dst_ref=there,
            send_sem=send_sem,
            recv_sem=recv_sem,
            device_id=(my_section, shard),
            device_id_type=MESH,
        )

    def along(block_chip, piece, target):
        block = block_chip * cores + core
        return copy(
            block, piece, target * cores + core, line_send.at[target], line_recv.at[block_chip, piece]
        )

    def over(block_chip, lane, piece):
        block = block_chip * cores + lane
        return copy(block, piece, chip * cores + pair, pair_send.at[block_chip], pair_recv.at[block_chip])

    def hand(block_chip, piece):
        if cores == 2:
            over(block_chip, core, piece).start()

    def send(i):
        far = chips - 1 - i
        for piece in range(pieces):

            @pl.when(chip + far < chips)
            def _():
                along(chip, piece, chip + far).start()

            @pl.when(chip - far >= 0)
            def _():
                along(chip, piece, chip - far).start()

    for_each(chips - 1, send)
    for piece in range(pieces):
        hand(chip, piece)

    def receive(i):
        for piece in range(pieces):

            @pl.when(chip - i - 1 >= 0)
            def _():
                along(chip - i - 1, piece, chip).wait_recv()
                hand(chip - i - 1, piece)

            @pl.when(chip + i + 1 < chips)
            def _():
                along(chip + i + 1, piece, chip).wait_recv()
                hand(chip + i + 1, piece)

    for_each(chips - 1, receive)

    def whole(block, sem):
        ref = weights.at[block]
        return pltpu.make_async_copy(ref, ref, sem)

    def finish(i):
        if cores == 2:
            whole(i * cores + pair, pair_recv.at[i]).wait()
            whole(i * cores + core, pair_send.at[i]).wait()

        @pl.when(i != chip)
        def _():
            whole(my_shard, line_send.at[i]).wait()

    for_each(chips, finish)
    pltpu.make_async_copy(others, others, part_send).wait()


def store_kernel(*refs):
    count = len(refs) // 2
    copies = [
        pltpu.make_async_copy(refs[i], refs[count + i], refs[-1].at[i]) for i in range(count)
    ]
    for copy in copies:
        copy.start()
    for copy in copies:
        copy.wait()


def local(sections, shards, master, first_moment, second_moment, gradient):
    _, rows, width = gradient.shape
    params = float(sections * shards * rows * width)
    total = sections * shards
    chips = shards // 2 if shards % 2 == 0 else shards
    pieces = PIECES if width % (PIECES * 128) == 0 else 1
    vmem = pl.BlockSpec(memory_space=pltpu.VMEM)
    hbm = pl.BlockSpec(memory_space=pltpu.HBM)
    results = [((1, rows, width), jnp.float32)] * 3
    results += [((shards, rows, width), jnp.bfloat16), ((1, 1), jnp.float32)]
    room = sum(math.prod(shape) * jnp.dtype(dtype).itemsize for shape, dtype in results)
    grant = min(GRANT_MOST, VMEM_MOST - room - rows * width * 2)
    held = pl.pallas_call(
        functools.partial(step_kernel, sections, shards, params, pieces),
        out_shape=tuple(pltpu.VMEM(shape, dtype) for shape, dtype in results),
        in_specs=[hbm] * 4,
        out_specs=(vmem,) * 5,
        scratch_shapes=[pltpu.VMEM((rows, width), jnp.float32)] * 4
        + [
            pltpu.VMEM((1, 128), jnp.float32),
            pltpu.VMEM((total, 128), jnp.float32),
            pltpu.SemaphoreType.DMA((4,)),
            pltpu.SemaphoreType.DMA,
            pltpu.SemaphoreType.DMA,
            pltpu.SemaphoreType.DMA((chips,)),
            pltpu.SemaphoreType.DMA((chips, pieces)),
            pltpu.SemaphoreType.DMA((chips,)),
            pltpu.SemaphoreType.DMA((chips,)),
        ],
        compiler_params=pltpu.CompilerParams(
            collective_id=0, has_side_effects=True, vmem_limit_bytes=grant
        ),
    )(master, first_moment, second_moment, gradient)
    new_master, new_first, new_second, weights, rms = pl.pallas_call(
        store_kernel,
        out_shape=tuple(jax.ShapeDtypeStruct(shape, dtype) for shape, dtype in results),
        in_specs=[vmem] * 5,
        out_specs=(hbm,) * 5,
        scratch_shapes=[pltpu.SemaphoreType.DMA((5,))],
        compiler_params=pltpu.CompilerParams(vmem_limit_bytes=grant),
    )(*[pltpu.with_memory_space_constraint(x, pltpu.VMEM) for x in held])
    return (
        new_master,
        new_first,
        new_second,
        weights.reshape(1, shards * rows, width),
        rms.reshape(()),
    )


def solution(mesh):
    placed = (P("section", "fsdp", None),) * 4
    return jax.shard_map(
        functools.partial(local, mesh.shape["section"], mesh.shape["fsdp"]),
        mesh=mesh,
        in_specs=placed,
        out_specs=(
            P("section", "fsdp", None),
            P("section", "fsdp", None),
            P("section", "fsdp", None),
            P("section", None, None),
            P(),
        ),
        check_vma=False,
    )
```

```python
import functools
import math

import jax
import jax.numpy as jnp
from jax import lax
from jax.experimental import pallas as pl
from jax.experimental.pallas import tpu as pltpu
from jax.sharding import PartitionSpec as P

BETA_ONE = 0.9
BETA_TWO = 0.95
LEARN_RATE = 0.05
DECAY = 0.1
EPSILON = 1e-08
BIAS_STEPS = 10.0
MESH = pl.DeviceIdType.MESH
UNROLL_MOST = 40
PIECES = 1
VMEM_MOST = 67043328
GRANT_MOST = 60 * 1024 * 1024


def for_each(count, body):
    if count <= UNROLL_MOST:
        for i in range(count):
            body(i)
    else:
        lax.fori_loop(0, count, lambda i, carry: (body(i), carry)[1], 0)


def step_kernel(
    sections, shards, params, pieces,
    master_hbm, first_hbm, second_hbm, grad_hbm,
    new_master, new_first, new_second, weights, rms,
    master, first, second, grad, part, parts,
    load_sem, part_send, part_recv, line_send, line_recv, pair_send, pair_recv,
):
    my_section = lax.axis_index("section")
    my_shard = lax.axis_index("fsdp")
    total = sections * shards
    me = my_section * shards + my_shard

    loads = [
        pltpu.make_async_copy(src.at[0], dst, load_sem.at[i])
        for i, (src, dst) in enumerate(
            ((grad_hbm, grad), (master_hbm, master), (first_hbm, first), (second_hbm, second))
        )
    ]
    loads[0].start()

    def peer(i):
        s = lax.rem(my_section + i // shards, sections)
        f = lax.rem(my_shard + i % shards, shards)
        return s, f

    barrier = pltpu.get_barrier_semaphore()

    def greet(i):
        pl.semaphore_signal(barrier, inc=1, device_id=peer(i + 1), device_id_type=MESH)

    for_each(total - 1, greet)

    for load in loads[1:]:
        load.start()

    loads[0].wait()
    g = grad[...]
    squares = g * g
    width = squares.shape[1]
    folded = squares[:, :128]
    for j in range(1, width // 128):
        folded += squares[:, j * 128 : (j + 1) * 128]
    row = jnp.sum(folded, axis=0, keepdims=True)
    part[...] = row
    parts[pl.ds(me, 1), :] = row

    pl.semaphore_wait(barrier, total - 1)

    def send_part(i):
        s, f = peer(i + 1)
        pltpu.make_async_remote_copy(
            src_ref=part,
            dst_ref=parts.at[pl.ds(me, 1)],
            send_sem=part_send,
            recv_sem=part_recv,
            device_id=(s, f),
            device_id_type=MESH,
        ).start()

    for_each(total - 1, send_part)
    for load in loads[1:]:
        load.wait()
    others = parts.at[pl.ds(0, total - 1)]
    pltpu.make_async_copy(others, others, part_recv).wait()

    squares_all = jnp.sum(jnp.sum(parts[...], axis=0, keepdims=True), axis=1, keepdims=True)
    norm = jnp.sqrt(squares_all)
    limit = jnp.float32(0.5 * params**0.5)
    clip = limit / jnp.maximum(norm, limit)
    rms[...] = jnp.broadcast_to(norm / jnp.float32(params**0.5), rms.shape)

    scaled = clip * g
    nf = BETA_ONE * first[...] + (1.0 - BETA_ONE) * scaled
    ns = BETA_TWO * second[...] + (1.0 - BETA_TWO) * scaled * scaled
    first_hat = nf / (1.0 - BETA_ONE**BIAS_STEPS)
    second_hat = ns / (1.0 - BETA_TWO**BIAS_STEPS)
    update = first_hat / (jnp.sqrt(second_hat) + EPSILON)
    nm = master[...] * (1.0 - LEARN_RATE * DECAY) - LEARN_RATE * update
    weights[my_shard] = nm.astype(jnp.bfloat16)
    new_master[0] = nm
    new_first[0] = nf
    new_second[0] = ns

    cores = 2 if shards % 2 == 0 else 1
    chips = shards // cores
    core = my_shard % cores
    chip = my_shard // cores
    pair = 1 - core
    cut = width // pieces

    def copy(block, piece, shard, send_sem, recv_sem):
        there = weights.at[block, :, pl.ds(piece * cut, cut)]
        return pltpu.make_async_remote_copy(
            src_ref=there,
            dst_ref=there,
            send_sem=send_sem,
            recv_sem=recv_sem,
            device_id=(my_section, shard),
            device_id_type=MESH,
        )

    def along(block_chip, piece, target):
        block = block_chip * cores + core
        return copy(
            block, piece, target * cores + core, line_send.at[target], line_recv.at[block_chip, piece]
        )

    def over(block_chip, lane, piece):
        block = block_chip * cores + lane
        return copy(block, piece, chip * cores + pair, pair_send.at[block_chip], pair_recv.at[block_chip])

    def hand(block_chip, piece):
        if cores == 2:
            over(block_chip, core, piece).start()

    def send(i):
        far = chips - 1 - i
        for piece in range(pieces):

            @pl.when(chip + far < chips)
            def _():
                along(chip, piece, chip + far).start()

            @pl.when(chip - far >= 0)
            def _():
                along(chip, piece, chip - far).start()

    for_each(chips - 1, send)
    for piece in range(pieces):
        hand(chip, piece)

    def receive(i):
        for piece in range(pieces):

            @pl.when(chip - i - 1 >= 0)
            def _():
                along(chip - i - 1, piece, chip).wait_recv()
                hand(chip - i - 1, piece)

            @pl.when(chip + i + 1 < chips)
            def _():
                along(chip + i + 1, piece, chip).wait_recv()
                hand(chip + i + 1, piece)

    for_each(chips - 1, receive)

    def whole(block, sem):
        ref = weights.at[block]
        return pltpu.make_async_copy(ref, ref, sem)

    def finish(i):
        if cores == 2:
            whole(i * cores + pair, pair_recv.at[i]).wait()
            whole(i * cores + core, pair_send.at[i]).wait()

        @pl.when(i != chip)
        def _():
            whole(my_shard, line_send.at[i]).wait()

    for_each(chips, finish)
    pltpu.make_async_copy(others, others, part_send).wait()


def store_kernel(*refs):
    held, outs, (rms, sem) = refs[:5], refs[5:10], refs[10:]
    copies = [pltpu.make_async_copy(held[i], outs[i], sem.at[i]) for i in range(4)]
    copies.append(pltpu.make_async_copy(rms, outs[4], sem.at[4]))
    for copy in copies[:4]:
        copy.start()
    rms[...] = held[4][:1, :1]
    copies[4].start()
    for copy in copies:
        copy.wait()


def local(sections, shards, master, first_moment, second_moment, gradient):
    _, rows, width = gradient.shape
    params = float(sections * shards * rows * width)
    total = sections * shards
    chips = shards // 2 if shards % 2 == 0 else shards
    pieces = PIECES if width % (PIECES * 128) == 0 else 1
    vmem = pl.BlockSpec(memory_space=pltpu.VMEM)
    hbm = pl.BlockSpec(memory_space=pltpu.HBM)
    results = [((1, rows, width), jnp.float32)] * 3
    results += [((shards, rows, width), jnp.bfloat16), ((8, 128), jnp.float32)]
    room = sum(math.prod(shape) * jnp.dtype(dtype).itemsize for shape, dtype in results)
    grant = min(GRANT_MOST, VMEM_MOST - room - rows * width * 2)
    held = pl.pallas_call(
        functools.partial(step_kernel, sections, shards, params, pieces),
        out_shape=tuple(pltpu.VMEM(shape, dtype) for shape, dtype in results),
        in_specs=[hbm] * 4,
        out_specs=(vmem,) * 5,
        scratch_shapes=[pltpu.VMEM((rows, width), jnp.float32)] * 4
        + [
            pltpu.VMEM((1, 128), jnp.float32),
            pltpu.VMEM((total, 128), jnp.float32),
            pltpu.SemaphoreType.DMA((4,)),
            pltpu.SemaphoreType.DMA,
            pltpu.SemaphoreType.DMA,
            pltpu.SemaphoreType.DMA((chips,)),
            pltpu.SemaphoreType.DMA((chips, pieces)),
            pltpu.SemaphoreType.DMA((chips,)),
            pltpu.SemaphoreType.DMA((chips,)),
        ],
        compiler_params=pltpu.CompilerParams(
            collective_id=0, has_side_effects=True, vmem_limit_bytes=grant
        ),
    )(master, first_moment, second_moment, gradient)
    new_master, new_first, new_second, weights, rms = pl.pallas_call(
        store_kernel,
        out_shape=tuple(jax.ShapeDtypeStruct(shape, dtype) for shape, dtype in results[:4])
        + (jax.ShapeDtypeStruct((1, 1), jnp.float32),),
        in_specs=[vmem] * 5,
        out_specs=(hbm,) * 5,
        scratch_shapes=[pltpu.VMEM((1, 1), jnp.float32), pltpu.SemaphoreType.DMA((5,))],
        compiler_params=pltpu.CompilerParams(vmem_limit_bytes=grant),
    )(*[pltpu.with_memory_space_constraint(x, pltpu.VMEM) for x in held])
    return (
        new_master,
        new_first,
        new_second,
        weights.reshape(1, shards * rows, width),
        rms.reshape(()),
    )


def solution(mesh):
    placed = (P("section", "fsdp", None),) * 4
    return jax.shard_map(
        functools.partial(local, mesh.shape["section"], mesh.shape["fsdp"]),
        mesh=mesh,
        in_specs=placed,
        out_specs=(
            P("section", "fsdp", None),
            P("section", "fsdp", None),
            P("section", "fsdp", None),
            P("section", None, None),
            P(),
        ),
        check_vma=False,
    )
```

```python
import functools
import math

import jax
import jax.numpy as jnp
from jax import lax
from jax.experimental import pallas as pl
from jax.experimental.pallas import tpu as pltpu
from jax.sharding import PartitionSpec as P

BETA_ONE = 0.9
BETA_TWO = 0.95
LEARN_RATE = 0.05
DECAY = 0.1
EPSILON = 1e-08
BIAS_STEPS = 10.0
MESH = pl.DeviceIdType.MESH
UNROLL_MOST = 40
PIECES = 1
VMEM_MOST = 67043328
GRANT_MOST = 60 * 1024 * 1024


def for_each(count, body):
    if count <= UNROLL_MOST:
        for i in range(count):
            body(i)
    else:
        lax.fori_loop(0, count, lambda i, carry: (body(i), carry)[1], 0)


def step_kernel(
    sections, shards, params, pieces,
    master_hbm, first_hbm, second_hbm, grad_hbm,
    new_master, new_first, new_second, weights, rms,
    master, first, second, grad, part, parts,
    load_sem, part_send, part_recv, line_send, pass_send, line_recv, pair_send, pair_recv,
):
    my_section = lax.axis_index("section")
    my_shard = lax.axis_index("fsdp")
    total = sections * shards
    me = my_section * shards + my_shard

    loads = [
        pltpu.make_async_copy(src.at[0], dst, load_sem.at[i])
        for i, (src, dst) in enumerate(
            ((grad_hbm, grad), (master_hbm, master), (first_hbm, first), (second_hbm, second))
        )
    ]
    loads[0].start()

    def peer(i):
        s = lax.rem(my_section + i // shards, sections)
        f = lax.rem(my_shard + i % shards, shards)
        return s, f

    barrier = pltpu.get_barrier_semaphore()

    def greet(i):
        pl.semaphore_signal(barrier, inc=1, device_id=peer(i + 1), device_id_type=MESH)

    for_each(total - 1, greet)

    for load in loads[1:]:
        load.start()

    loads[0].wait()
    g = grad[...]
    squares = g * g
    width = squares.shape[1]
    folded = squares[:, :128]
    for j in range(1, width // 128):
        folded += squares[:, j * 128 : (j + 1) * 128]
    row = jnp.sum(folded, axis=0, keepdims=True)
    part[...] = row
    parts[pl.ds(me, 1), :] = row

    pl.semaphore_wait(barrier, total - 1)

    def send_part(i):
        s, f = peer(i + 1)
        pltpu.make_async_remote_copy(
            src_ref=part,
            dst_ref=parts.at[pl.ds(me, 1)],
            send_sem=part_send,
            recv_sem=part_recv,
            device_id=(s, f),
            device_id_type=MESH,
        ).start()

    for_each(total - 1, send_part)
    for load in loads[1:]:
        load.wait()
    others = parts.at[pl.ds(0, total - 1)]
    pltpu.make_async_copy(others, others, part_recv).wait()

    squares_all = jnp.sum(jnp.sum(parts[...], axis=0, keepdims=True), axis=1, keepdims=True)
    norm = jnp.sqrt(squares_all)
    limit = jnp.float32(0.5 * params**0.5)
    clip = limit / jnp.maximum(norm, limit)
    rms[...] = jnp.broadcast_to(norm / jnp.float32(params**0.5), rms.shape)

    scaled = clip * g
    nf = BETA_ONE * first[...] + (1.0 - BETA_ONE) * scaled
    ns = BETA_TWO * second[...] + (1.0 - BETA_TWO) * scaled * scaled
    first_hat = nf / (1.0 - BETA_ONE**BIAS_STEPS)
    second_hat = ns / (1.0 - BETA_TWO**BIAS_STEPS)
    update = first_hat / (jnp.sqrt(second_hat) + EPSILON)
    nm = master[...] * (1.0 - LEARN_RATE * DECAY) - LEARN_RATE * update
    weights[my_shard] = nm.astype(jnp.bfloat16)
    new_master[0] = nm
    new_first[0] = nf
    new_second[0] = ns

    cores = 2 if shards % 2 == 0 else 1
    chips = shards // cores
    core = my_shard % cores
    chip = my_shard // cores
    pair = 1 - core
    cut = width // pieces

    def copy(block, piece, shard, send_sem, recv_sem):
        there = weights.at[block, :, pl.ds(piece * cut, cut)]
        return pltpu.make_async_remote_copy(
            src_ref=there,
            dst_ref=there,
            send_sem=send_sem,
            recv_sem=recv_sem,
            device_id=(my_section, shard),
            device_id_type=MESH,
        )

    def along(block_chip, piece, target, sends):
        block = block_chip * cores + core
        return copy(
            block, piece, target * cores + core, sends.at[target], line_recv.at[block_chip, piece]
        )

    def over(block_chip, lane, piece):
        block = block_chip * cores + lane
        return copy(block, piece, chip * cores + pair, pair_send.at[block_chip], pair_recv.at[block_chip])

    def hand(block_chip, piece):
        if cores == 2:
            over(block_chip, core, piece).start()

    half = chips // 2
    above_mid = jnp.logical_and(chip == half, core == cores - 1)
    below_mid = jnp.logical_and(chip == half - 1, core == cores - 1)

    def direct(target):
        return jnp.logical_not(jnp.logical_and(above_mid, target < half - 1))

    def send(i):
        far = chips - 1 - i
        for piece in range(pieces):

            @pl.when(jnp.logical_and(chip + far < chips, direct(chip + far)))
            def _():
                along(chip, piece, chip + far, line_send).start()

            @pl.when(jnp.logical_and(chip - far >= 0, direct(chip - far)))
            def _():
                along(chip, piece, chip - far, line_send).start()

    for_each(chips - 1, send)
    for piece in range(pieces):
        hand(chip, piece)

    for piece in range(pieces):

        @pl.when(below_mid)
        def _():
            along(half, piece, chip, line_send).wait_recv()
            for_each(half - 1, lambda j: along(half, piece, j, pass_send).start())
            hand(half, piece)

    def receive(i):
        for piece in range(pieces):
            below, above = chip - i - 1, chip + i + 1

            @pl.when(below >= 0)
            def _():
                along(below, piece, chip, line_send).wait_recv()
                hand(below, piece)

            @pl.when(jnp.logical_and(above < chips, jnp.logical_not(jnp.logical_and(below_mid, i == 0))))
            def _():
                along(above, piece, chip, line_send).wait_recv()
                hand(above, piece)

    for_each(chips - 1, receive)

    def whole(block, sem):
        ref = weights.at[block]
        return pltpu.make_async_copy(ref, ref, sem)

    def finish(i):
        if cores == 2:
            whole(i * cores + pair, pair_recv.at[i]).wait()
            whole(i * cores + core, pair_send.at[i]).wait()

        @pl.when(jnp.logical_and(i != chip, direct(i)))
        def _():
            whole(my_shard, line_send.at[i]).wait()

        @pl.when(jnp.logical_and(below_mid, i < half - 1))
        def _():
            whole(my_shard, pass_send.at[i]).wait()

    for_each(chips, finish)
    pltpu.make_async_copy(others, others, part_send).wait()


def store_kernel(*refs):
    held, outs, (rms, sem) = refs[:5], refs[5:10], refs[10:]
    copies = [pltpu.make_async_copy(held[i], outs[i], sem.at[i]) for i in range(4)]
    copies.append(pltpu.make_async_copy(rms, outs[4], sem.at[4]))
    for copy in copies[:4]:
        copy.start()
    rms[...] = held[4][:1, :1]
    copies[4].start()
    for copy in copies:
        copy.wait()


def local(sections, shards, master, first_moment, second_moment, gradient):
    _, rows, width = gradient.shape
    params = float(sections * shards * rows * width)
    total = sections * shards
    chips = shards // 2 if shards % 2 == 0 else shards
    pieces = PIECES if width % (PIECES * 128) == 0 else 1
    vmem = pl.BlockSpec(memory_space=pltpu.VMEM)
    hbm = pl.BlockSpec(memory_space=pltpu.HBM)
    results = [((1, rows, width), jnp.float32)] * 3
    results += [((shards, rows, width), jnp.bfloat16), ((8, 128), jnp.float32)]
    room = sum(math.prod(shape) * jnp.dtype(dtype).itemsize for shape, dtype in results)
    grant = min(GRANT_MOST, VMEM_MOST - room - rows * width * 2)
    held = pl.pallas_call(
        functools.partial(step_kernel, sections, shards, params, pieces),
        out_shape=tuple(pltpu.VMEM(shape, dtype) for shape, dtype in results),
        in_specs=[hbm] * 4,
        out_specs=(vmem,) * 5,
        scratch_shapes=[pltpu.VMEM((rows, width), jnp.float32)] * 4
        + [
            pltpu.VMEM((1, 128), jnp.float32),
            pltpu.VMEM((total, 128), jnp.float32),
            pltpu.SemaphoreType.DMA((4,)),
            pltpu.SemaphoreType.DMA,
            pltpu.SemaphoreType.DMA,
            pltpu.SemaphoreType.DMA((chips,)),
            pltpu.SemaphoreType.DMA((chips,)),
            pltpu.SemaphoreType.DMA((chips, pieces)),
            pltpu.SemaphoreType.DMA((chips,)),
            pltpu.SemaphoreType.DMA((chips,)),
        ],
        compiler_params=pltpu.CompilerParams(
            collective_id=0, has_side_effects=True, vmem_limit_bytes=grant
        ),
    )(master, first_moment, second_moment, gradient)
    new_master, new_first, new_second, weights, rms = pl.pallas_call(
        store_kernel,
        out_shape=tuple(jax.ShapeDtypeStruct(shape, dtype) for shape, dtype in results[:4])
        + (jax.ShapeDtypeStruct((1, 1), jnp.float32),),
        in_specs=[vmem] * 5,
        out_specs=(hbm,) * 5,
        scratch_shapes=[pltpu.VMEM((1, 1), jnp.float32), pltpu.SemaphoreType.DMA((5,))],
        compiler_params=pltpu.CompilerParams(vmem_limit_bytes=grant),
    )(*[pltpu.with_memory_space_constraint(x, pltpu.VMEM) for x in held])
    return (
        new_master,
        new_first,
        new_second,
        weights.reshape(1, shards * rows, width),
        rms.reshape(()),
    )


def solution(mesh):
    placed = (P("section", "fsdp", None),) * 4
    return jax.shard_map(
        functools.partial(local, mesh.shape["section"], mesh.shape["fsdp"]),
        mesh=mesh,
        in_specs=placed,
        out_specs=(
            P("section", "fsdp", None),
            P("section", "fsdp", None),
            P("section", "fsdp", None),
            P("section", None, None),
            P(),
        ),
        check_vma=False,
    )
```

```python
import functools
import math

import jax
import jax.numpy as jnp
from jax import lax
from jax.experimental import pallas as pl
from jax.experimental.pallas import tpu as pltpu
from jax.sharding import PartitionSpec as P

BETA_ONE = 0.9
BETA_TWO = 0.95
LEARN_RATE = 0.05
DECAY = 0.1
EPSILON = 1e-08
BIAS_STEPS = 10.0
MESH = pl.DeviceIdType.MESH
UNROLL_MOST = 40
PIECES = 2
VMEM_MOST = 67043328
GRANT_MOST = 60 * 1024 * 1024


def for_each(count, body):
    if count <= UNROLL_MOST:
        for i in range(count):
            body(i)
    else:
        lax.fori_loop(0, count, lambda i, carry: (body(i), carry)[1], 0)


def step_kernel(
    sections, shards, params, pieces,
    master_hbm, first_hbm, second_hbm, grad_hbm,
    new_master, new_first, new_second, weights, rms,
    master, first, second, grad, part, parts,
    load_sem, part_send, part_recv, line_send, pass_send, next_send, line_recv, pair_send, pair_recv,
):
    my_section = lax.axis_index("section")
    my_shard = lax.axis_index("fsdp")
    total = sections * shards
    me = my_section * shards + my_shard

    loads = [
        pltpu.make_async_copy(src.at[0], dst, load_sem.at[i])
        for i, (src, dst) in enumerate(
            ((grad_hbm, grad), (master_hbm, master), (first_hbm, first), (second_hbm, second))
        )
    ]
    loads[0].start()

    def peer(i):
        i = i - 1
        step = i // sections
        turn = shards // 2 + (step + 1) // 2 * (1 - 2 * (step % 2))
        s = lax.rem(my_section + sections - 1 - i % sections, sections)
        f = lax.rem(my_shard + turn + shards, shards)
        return s, f

    barrier = pltpu.get_barrier_semaphore()

    def greet(i):
        pl.semaphore_signal(barrier, inc=1, device_id=peer(i + 1), device_id_type=MESH)

    for_each(total - 1, greet)

    for load in loads[1:]:
        load.start()

    loads[0].wait()
    g = grad[...]
    squares = g * g
    width = squares.shape[1]
    folded = squares[:, :128]
    for j in range(1, width // 128):
        folded += squares[:, j * 128 : (j + 1) * 128]
    row = jnp.sum(folded, axis=0, keepdims=True)
    part[...] = row
    parts[pl.ds(me, 1), :] = row

    pl.semaphore_wait(barrier, total - 1)

    def send_part(i):
        s, f = peer(i + 1)
        pltpu.make_async_remote_copy(
            src_ref=part,
            dst_ref=parts.at[pl.ds(me, 1)],
            send_sem=part_send,
            recv_sem=part_recv,
            device_id=(s, f),
            device_id_type=MESH,
        ).start()

    for_each(total - 1, send_part)
    for load in loads[1:]:
        load.wait()
    others = parts.at[pl.ds(0, total - 1)]
    pltpu.make_async_copy(others, others, part_recv).wait()

    squares_all = jnp.sum(jnp.sum(parts[...], axis=0, keepdims=True), axis=1, keepdims=True)
    norm = jnp.sqrt(squares_all)
    limit = jnp.float32(0.5 * params**0.5)
    clip = limit / jnp.maximum(norm, limit)
    rms[...] = jnp.broadcast_to(norm / jnp.float32(params**0.5), rms.shape)

    scaled = clip * g
    nf = BETA_ONE * first[...] + (1.0 - BETA_ONE) * scaled
    ns = BETA_TWO * second[...] + (1.0 - BETA_TWO) * scaled * scaled
    first_hat = nf / (1.0 - BETA_ONE**BIAS_STEPS)
    second_hat = ns / (1.0 - BETA_TWO**BIAS_STEPS)
    update = first_hat / (jnp.sqrt(second_hat) + EPSILON)
    nm = master[...] * (1.0 - LEARN_RATE * DECAY) - LEARN_RATE * update
    weights[my_shard] = nm.astype(jnp.bfloat16)
    new_master[0] = nm
    new_first[0] = nf
    new_second[0] = ns

    cores = 2 if shards % 2 == 0 else 1
    chips = shards // cores
    core = my_shard % cores
    chip = my_shard // cores
    pair = 1 - core
    cut = width // pieces

    def copy(block, piece, shard, send_sem, recv_sem):
        there = weights.at[block, :, pl.ds(piece * cut, cut)]
        return pltpu.make_async_remote_copy(
            src_ref=there,
            dst_ref=there,
            send_sem=send_sem,
            recv_sem=recv_sem,
            device_id=(my_section, shard),
            device_id_type=MESH,
        )

    def along(block_chip, piece, target, sends):
        block = block_chip * cores + core
        return copy(
            block, piece, target * cores + core, sends.at[target], line_recv.at[block_chip, piece]
        )

    def over(block_chip, lane, piece):
        block = block_chip * cores + lane
        return copy(block, piece, chip * cores + pair, pair_send.at[block_chip], pair_recv.at[block_chip])

    def hand(block_chip, piece):
        if cores == 2:
            over(block_chip, core, piece).start()

    half = chips // 2
    right_source = jnp.logical_and(chip == half - 2, core == cores - 1)
    left_source = jnp.logical_and(
        jnp.logical_or(chip == half, chip == half + 1), core == cores - 1
    )
    above_mid = jnp.logical_and(chip == half, core == cores - 1)
    below_mid = jnp.logical_and(chip == half - 1, core == cores - 1)

    def direct(target):
        right = jnp.logical_and(right_source, target > half)
        left = jnp.logical_and(left_source, target < half - 1)
        return jnp.logical_not(jnp.logical_or(right, left))

    def send(i):
        far = chips - 1 - i
        for piece in range(pieces):

            @pl.when(jnp.logical_and(chip + far < chips, direct(chip + far)))
            def _():
                along(chip, piece, chip + far, line_send).start()

            @pl.when(jnp.logical_and(chip - far >= 0, direct(chip - far)))
            def _():
                along(chip, piece, chip - far, line_send).start()

    for_each(chips - 1, send)
    for piece in range(pieces):
        hand(chip, piece)

    for piece in range(pieces):

        @pl.when(above_mid)
        def _():
            if half > 1:
                along(half - 2, piece, chip, line_send).wait_recv()
                for_each(
                    chips - 1 - half,
                    lambda j: along(half - 2, piece, chips - 1 - j, pass_send).start(),
                )
                hand(half - 2, piece)

        @pl.when(below_mid)
        def _():
            for source, sends in ((half, pass_send), (half + 1, next_send)):
                if source < chips:
                    along(source, piece, chip, line_send).wait_recv()
                    for_each(half - 1, lambda j: along(source, piece, j, sends).start())
                    hand(source, piece)

    def receive(i):
        for piece in range(pieces):
            below, above = chip - i - 1, chip + i + 1

            @pl.when(jnp.logical_and(below >= 0, jnp.logical_not(jnp.logical_and(above_mid, i == 1))))
            def _():
                along(below, piece, chip, line_send).wait_recv()
                hand(below, piece)

            @pl.when(jnp.logical_and(above < chips, jnp.logical_not(jnp.logical_and(below_mid, i < 2))))
            def _():
                along(above, piece, chip, line_send).wait_recv()
                hand(above, piece)

    for_each(chips - 1, receive)

    def whole(block, sem):
        ref = weights.at[block]
        return pltpu.make_async_copy(ref, ref, sem)

    def finish(i):
        if cores == 2:
            whole(i * cores + pair, pair_recv.at[i]).wait()
            whole(i * cores + core, pair_send.at[i]).wait()

        @pl.when(jnp.logical_and(i != chip, direct(i)))
        def _():
            whole(my_shard, line_send.at[i]).wait()

        @pl.when(jnp.logical_or(jnp.logical_and(above_mid, jnp.logical_and(i > half, half > 1)), jnp.logical_and(below_mid, i < half - 1)))
        def _():
            whole(my_shard, pass_send.at[i]).wait()

        if half + 1 < chips:

            @pl.when(jnp.logical_and(below_mid, i < half - 1))
            def _():
                whole(my_shard, next_send.at[i]).wait()

    for_each(chips, finish)
    pltpu.make_async_copy(others, others, part_send).wait()


def store_kernel(*refs):
    held, outs, (rms, sem) = refs[:5], refs[5:10], refs[10:]
    copies = [pltpu.make_async_copy(held[i], outs[i], sem.at[i]) for i in range(4)]
    copies.append(pltpu.make_async_copy(rms, outs[4], sem.at[4]))
    for copy in copies[:4]:
        copy.start()
    rms[...] = held[4][:1, :1]
    copies[4].start()
    for copy in copies:
        copy.wait()


def local(sections, shards, master, first_moment, second_moment, gradient):
    _, rows, width = gradient.shape
    params = float(sections * shards * rows * width)
    total = sections * shards
    chips = shards // 2 if shards % 2 == 0 else shards
    pieces = PIECES if width % (PIECES * 128) == 0 else 1
    vmem = pl.BlockSpec(memory_space=pltpu.VMEM)
    hbm = pl.BlockSpec(memory_space=pltpu.HBM)
    results = [((1, rows, width), jnp.float32)] * 3
    results += [((shards, rows, width), jnp.bfloat16), ((8, 128), jnp.float32)]
    room = sum(math.prod(shape) * jnp.dtype(dtype).itemsize for shape, dtype in results)
    grant = min(GRANT_MOST, VMEM_MOST - room - rows * width * 2)
    held = pl.pallas_call(
        functools.partial(step_kernel, sections, shards, params, pieces),
        out_shape=tuple(pltpu.VMEM(shape, dtype) for shape, dtype in results),
        in_specs=[hbm] * 4,
        out_specs=(vmem,) * 5,
        scratch_shapes=[pltpu.VMEM((rows, width), jnp.float32)] * 4
        + [
            pltpu.VMEM((1, 128), jnp.float32),
            pltpu.VMEM((total, 128), jnp.float32),
            pltpu.SemaphoreType.DMA((4,)),
            pltpu.SemaphoreType.DMA,
            pltpu.SemaphoreType.DMA,
            pltpu.SemaphoreType.DMA((chips,)),
            pltpu.SemaphoreType.DMA((chips,)),
            pltpu.SemaphoreType.DMA((chips,)),
            pltpu.SemaphoreType.DMA((chips, pieces)),
            pltpu.SemaphoreType.DMA((chips,)),
            pltpu.SemaphoreType.DMA((chips,)),
        ],
        compiler_params=pltpu.CompilerParams(
            collective_id=0, has_side_effects=True, vmem_limit_bytes=grant
        ),
    )(master, first_moment, second_moment, gradient)
    new_master, new_first, new_second, weights, rms = pl.pallas_call(
        store_kernel,
        out_shape=tuple(jax.ShapeDtypeStruct(shape, dtype) for shape, dtype in results[:4])
        + (jax.ShapeDtypeStruct((1, 1), jnp.float32),),
        in_specs=[vmem] * 5,
        out_specs=(hbm,) * 5,
        scratch_shapes=[pltpu.VMEM((1, 1), jnp.float32), pltpu.SemaphoreType.DMA((5,))],
        compiler_params=pltpu.CompilerParams(vmem_limit_bytes=grant),
    )(*[pltpu.with_memory_space_constraint(x, pltpu.VMEM) for x in held])
    return (
        new_master,
        new_first,
        new_second,
        weights.reshape(1, shards * rows, width),
        rms.reshape(()),
    )


def solution(mesh):
    placed = (P("section", "fsdp", None),) * 4
    return jax.shard_map(
        functools.partial(local, mesh.shape["section"], mesh.shape["fsdp"]),
        mesh=mesh,
        in_specs=placed,
        out_specs=(
            P("section", "fsdp", None),
            P("section", "fsdp", None),
            P("section", "fsdp", None),
            P("section", None, None),
            P(),
        ),
        check_vma=False,
    )
```

```python
import functools
import math

import jax
import jax.numpy as jnp
from jax import lax
from jax.experimental import pallas as pl
from jax.experimental.pallas import tpu as pltpu
from jax.sharding import PartitionSpec as P

BETA_ONE = 0.9
BETA_TWO = 0.95
LEARN_RATE = 0.05
DECAY = 0.1
EPSILON = 1e-08
BIAS_STEPS = 10.0
MESH = pl.DeviceIdType.MESH
UNROLL_MOST = 40
PIECES = 2
VMEM_MOST = 67043328
GRANT_MOST = 60 * 1024 * 1024


def for_each(count, body):
    if count <= UNROLL_MOST:
        for i in range(count):
            body(i)
    else:
        lax.fori_loop(0, count, lambda i, carry: (body(i), carry)[1], 0)


def step_kernel(
    sections, shards, params, pieces,
    master_hbm, first_hbm, second_hbm, grad_hbm,
    new_master, new_first, new_second, weights, rms,
    master, first, second, grad, part, parts,
    load_sem, part_send, part_recv, line_send, pass_send, next_send, line_recv, pair_send, pair_recv,
):
    my_section = lax.axis_index("section")
    my_shard = lax.axis_index("fsdp")
    total = sections * shards
    me = my_section * shards + my_shard

    loads = [
        pltpu.make_async_copy(src.at[0], dst, load_sem.at[i])
        for i, (src, dst) in enumerate(
            ((grad_hbm, grad), (master_hbm, master), (first_hbm, first), (second_hbm, second))
        )
    ]
    loads[0].start()

    def peer(i):
        i = i - 1
        step = i // sections
        turn = shards // 2 + (step + 1) // 2 * (1 - 2 * (step % 2))
        s = lax.rem(my_section + sections - 1 - i % sections, sections)
        f = lax.rem(my_shard + turn + shards, shards)
        return s, f

    barrier = pltpu.get_barrier_semaphore()

    def greet(i):
        pl.semaphore_signal(barrier, inc=1, device_id=peer(i + 1), device_id_type=MESH)

    for_each(total - 1, greet)

    for load in loads[1:]:
        load.start()

    loads[0].wait()
    g = grad[...]
    squares = g * g
    width = squares.shape[1]
    folded = squares[:, :128]
    for j in range(1, width // 128):
        folded += squares[:, j * 128 : (j + 1) * 128]
    row = jnp.sum(folded, axis=0, keepdims=True)
    part[...] = row
    parts[pl.ds(me, 1), :] = row

    pl.semaphore_wait(barrier, total - 1)

    def send_part(i):
        s, f = peer(i + 1)
        pltpu.make_async_remote_copy(
            src_ref=part,
            dst_ref=parts.at[pl.ds(me, 1)],
            send_sem=part_send,
            recv_sem=part_recv,
            device_id=(s, f),
            device_id_type=MESH,
        ).start()

    for_each(total - 1, send_part)
    for load in loads[1:]:
        load.wait()
    others = parts.at[pl.ds(0, total - 1)]
    pltpu.make_async_copy(others, others, part_recv).wait()

    squares_all = jnp.sum(jnp.sum(parts[...], axis=0, keepdims=True), axis=1, keepdims=True)
    norm = jnp.sqrt(squares_all)
    limit = jnp.float32(0.5 * params**0.5)
    clip = limit / jnp.maximum(norm, limit)
    rms[...] = jnp.broadcast_to(norm / jnp.float32(params**0.5), rms.shape)

    scaled = clip * g
    nf = BETA_ONE * first[...] + (1.0 - BETA_ONE) * scaled
    ns = BETA_TWO * second[...] + (1.0 - BETA_TWO) * scaled * scaled
    first_hat = nf / (1.0 - BETA_ONE**BIAS_STEPS)
    second_hat = ns / (1.0 - BETA_TWO**BIAS_STEPS)
    update = first_hat / (jnp.sqrt(second_hat) + EPSILON)
    nm = master[...] * (1.0 - LEARN_RATE * DECAY) - LEARN_RATE * update
    weights[my_shard] = nm.astype(jnp.bfloat16)
    cores = 2 if shards % 2 == 0 else 1
    chips = shards // cores
    core = my_shard % cores
    chip = my_shard // cores
    pair = 1 - core
    cut = width // pieces

    def copy(block, piece, shard, send_sem, recv_sem):
        there = weights.at[block, :, pl.ds(piece * cut, cut)]
        return pltpu.make_async_remote_copy(
            src_ref=there,
            dst_ref=there,
            send_sem=send_sem,
            recv_sem=recv_sem,
            device_id=(my_section, shard),
            device_id_type=MESH,
        )

    def along(block_chip, piece, target, sends):
        block = block_chip * cores + core
        return copy(
            block, piece, target * cores + core, sends.at[target], line_recv.at[block_chip, piece]
        )

    def over(block_chip, lane, piece):
        block = block_chip * cores + lane
        return copy(block, piece, chip * cores + pair, pair_send.at[block_chip], pair_recv.at[block_chip])

    def hand(block_chip, piece):
        if cores == 2:
            over(block_chip, core, piece).start()

    half = chips // 2
    right_source = jnp.logical_and(chip == half - 2, core == cores - 1)
    left_source = jnp.logical_and(
        jnp.logical_or(chip == half, chip == half + 1), core == cores - 1
    )
    above_mid = jnp.logical_and(chip == half, core == cores - 1)
    below_mid = jnp.logical_and(chip == half - 1, core == cores - 1)

    def direct(target):
        right = jnp.logical_and(right_source, target > half)
        left = jnp.logical_and(left_source, target < half - 1)
        return jnp.logical_not(jnp.logical_or(right, left))

    def send(i):
        far = chips - 1 - i
        for piece in range(pieces):

            @pl.when(jnp.logical_and(chip + far < chips, direct(chip + far)))
            def _():
                along(chip, piece, chip + far, line_send).start()

            @pl.when(jnp.logical_and(chip - far >= 0, direct(chip - far)))
            def _():
                along(chip, piece, chip - far, line_send).start()

    for_each(chips - 1, send)
    for piece in range(pieces):
        hand(chip, piece)

    new_master[0] = nm
    new_first[0] = nf
    new_second[0] = ns

    for piece in range(pieces):

        @pl.when(above_mid)
        def _():
            if half > 1:
                along(half - 2, piece, chip, line_send).wait_recv()
                for_each(
                    chips - 1 - half,
                    lambda j: along(half - 2, piece, chips - 1 - j, pass_send).start(),
                )
                hand(half - 2, piece)

        @pl.when(below_mid)
        def _():
            for source, sends in ((half, pass_send), (half + 1, next_send)):
                if source < chips:
                    along(source, piece, chip, line_send).wait_recv()
                    for_each(half - 1, lambda j: along(source, piece, j, sends).start())
                    hand(source, piece)

    def receive(i):
        i = jnp.where(core == cores - 1, i, chips - 2 - i)
        for piece in range(pieces):
            below, above = chip - i - 1, chip + i + 1

            @pl.when(jnp.logical_and(below >= 0, jnp.logical_not(jnp.logical_and(above_mid, i == 1))))
            def _():
                along(below, piece, chip, line_send).wait_recv()
                hand(below, piece)

            @pl.when(jnp.logical_and(above < chips, jnp.logical_not(jnp.logical_and(below_mid, i < 2))))
            def _():
                along(above, piece, chip, line_send).wait_recv()
                hand(above, piece)

    for_each(chips - 1, receive)

    def whole(block, sem):
        ref = weights.at[block]
        return pltpu.make_async_copy(ref, ref, sem)

    def finish(i):
        if cores == 2:
            whole(i * cores + pair, pair_recv.at[i]).wait()
            whole(i * cores + core, pair_send.at[i]).wait()

        @pl.when(jnp.logical_and(i != chip, direct(i)))
        def _():
            whole(my_shard, line_send.at[i]).wait()

        @pl.when(jnp.logical_or(jnp.logical_and(above_mid, jnp.logical_and(i > half, half > 1)), jnp.logical_and(below_mid, i < half - 1)))
        def _():
            whole(my_shard, pass_send.at[i]).wait()

        if half + 1 < chips:

            @pl.when(jnp.logical_and(below_mid, i < half - 1))
            def _():
                whole(my_shard, next_send.at[i]).wait()

    for_each(chips, finish)
    pltpu.make_async_copy(others, others, part_send).wait()


def store_kernel(*refs):
    held, outs, (rms, sem) = refs[:5], refs[5:10], refs[10:]
    copies = [pltpu.make_async_copy(held[i], outs[i], sem.at[i]) for i in range(4)]
    copies.append(pltpu.make_async_copy(rms, outs[4], sem.at[4]))
    for copy in copies[:4]:
        copy.start()
    rms[...] = held[4][:1, :1]
    copies[4].start()
    for copy in copies:
        copy.wait()


def local(sections, shards, master, first_moment, second_moment, gradient):
    _, rows, width = gradient.shape
    params = float(sections * shards * rows * width)
    total = sections * shards
    chips = shards // 2 if shards % 2 == 0 else shards
    pieces = PIECES if width % (PIECES * 128) == 0 else 1
    vmem = pl.BlockSpec(memory_space=pltpu.VMEM)
    hbm = pl.BlockSpec(memory_space=pltpu.HBM)
    results = [((1, rows, width), jnp.float32)] * 3
    results += [((shards, rows, width), jnp.bfloat16), ((8, 128), jnp.float32)]
    room = sum(math.prod(shape) * jnp.dtype(dtype).itemsize for shape, dtype in results)
    grant = min(GRANT_MOST, VMEM_MOST - room - rows * width * 2)
    held = pl.pallas_call(
        functools.partial(step_kernel, sections, shards, params, pieces),
        out_shape=tuple(pltpu.VMEM(shape, dtype) for shape, dtype in results),
        in_specs=[hbm] * 4,
        out_specs=(vmem,) * 5,
        scratch_shapes=[pltpu.VMEM((rows, width), jnp.float32)] * 4
        + [
            pltpu.VMEM((1, 128), jnp.float32),
            pltpu.VMEM((total, 128), jnp.float32),
            pltpu.SemaphoreType.DMA((4,)),
            pltpu.SemaphoreType.DMA,
            pltpu.SemaphoreType.DMA,
            pltpu.SemaphoreType.DMA((chips,)),
            pltpu.SemaphoreType.DMA((chips,)),
            pltpu.SemaphoreType.DMA((chips,)),
            pltpu.SemaphoreType.DMA((chips, pieces)),
            pltpu.SemaphoreType.DMA((chips,)),
            pltpu.SemaphoreType.DMA((chips,)),
        ],
        compiler_params=pltpu.CompilerParams(
            collective_id=0, has_side_effects=True, vmem_limit_bytes=grant
        ),
    )(master, first_moment, second_moment, gradient)
    new_master, new_first, new_second, weights, rms = pl.pallas_call(
        store_kernel,
        out_shape=tuple(jax.ShapeDtypeStruct(shape, dtype) for shape, dtype in results[:4])
        + (jax.ShapeDtypeStruct((1, 1), jnp.float32),),
        in_specs=[vmem] * 5,
        out_specs=(hbm,) * 5,
        scratch_shapes=[pltpu.VMEM((1, 1), jnp.float32), pltpu.SemaphoreType.DMA((5,))],
        compiler_params=pltpu.CompilerParams(vmem_limit_bytes=grant),
    )(*[pltpu.with_memory_space_constraint(x, pltpu.VMEM) for x in held])
    return (
        new_master,
        new_first,
        new_second,
        weights.reshape(1, shards * rows, width),
        rms.reshape(()),
    )


def solution(mesh):
    placed = (P("section", "fsdp", None),) * 4
    return jax.shard_map(
        functools.partial(local, mesh.shape["section"], mesh.shape["fsdp"]),
        mesh=mesh,
        in_specs=placed,
        out_specs=(
            P("section", "fsdp", None),
            P("section", "fsdp", None),
            P("section", "fsdp", None),
            P("section", None, None),
            P(),
        ),
        check_vma=False,
    )
```
